64 devices in a mesh: dp: 8 (over x, y, core), tp: 8 (over z).
Axes of the slice: x: 2, y: 2, z: 8, core: 2. Of those that a mesh axis runs over, the one named last changes fastest.
The devices are a block of a 4x4x8 slice.
Arguments:
- x: bfloat16 [16384, 2048], P('dp'), parts along dimension 0
- dy: bfloat16 [16384, 2048], P('dp'), parts along dimension 0
- gate: bfloat16 [16384, 16384], P('dp', 'tp'), parts along dimension 0
- up: bfloat16 [16384, 16384], P('dp', 'tp'), parts along dimension 0
- w_gate: bfloat16 [2048, 16384], P(None, 'tp')
- w_up: bfloat16 [2048, 16384], P(None, 'tp')
- w_down: bfloat16 [16384, 2048], P('tp')
Outputs:
- output 1: bfloat16 [16384, 2048], P('dp'), parts along dimension 0
- output 2: bfloat16 [16384, 16384], P('dp', 'tp'), parts along dimension 0
- output 3: bfloat16 [16384, 16384], P('dp', 'tp'), parts along dimension 0
- output 4: bfloat16 [131072, 2048], P(('dp', 'tp')), parts along dimension 0
There are 8 independent parts. The reference program is written for one: setup_inputs(seed, part) draws one part's arguments, and reference() takes and returns one part's arrays. A program takes and returns all parts, laid end to end along the dimension named above; an argument that names none is the same for every part.
All inputs are finite; a program needn't handle non-finite values.
Results may differ from the reference program's by a relative error of at most 0.012.
Values are sent between devices in bfloat16 or wider.
A program may use at most 768 MiB of HBM per device.

```python
import jax
import jax.numpy as jnp

ROWS = 2048
D = 2048
FF = 16384


def act(gate, up):
    return jax.nn.gelu(gate) * up


def setup_inputs(seed: int = 0, part: int = 0) -> dict:
    kx, ky, ka, kb, kg, ku, kd = jax.random.split(jax.random.key(seed), 7)
    kx, ky, ka, kb = (jax.random.fold_in(k, part) for k in (kx, ky, ka, kb))
    drawn = {
        "x": jax.random.normal(kx, (ROWS, D), jnp.float32),
        "dy": jax.random.normal(ky, (ROWS, D), jnp.float32),
        "gate": jax.random.normal(ka, (ROWS, FF), jnp.float32),
        "up": jax.random.normal(kb, (ROWS, FF), jnp.float32),
        "w_gate": jax.random.normal(kg, (D, FF), jnp.float32) * D**-0.5,
        "w_up": jax.random.normal(ku, (D, FF), jnp.float32) * D**-0.5,
        "w_down": jax.random.normal(kd, (FF, D), jnp.float32) * FF**-0.5,
    }
    return {k: v.astype(jnp.bfloat16) for k, v in drawn.items()}


def reference(x, dy, gate, up, w_gate, w_up, w_down):
    hidden, back = jax.vjp(act, gate.astype(jnp.float32), up.astype(jnp.float32))
    d_hidden = jnp.dot(dy, w_down.T, preferred_element_type=jnp.float32)
    d_gate, d_up = (g.astype(jnp.bfloat16) for g in back(d_hidden))
    dx = jnp.dot(d_gate, w_gate.T, preferred_element_type=jnp.float32) + jnp.dot(d_up, w_up.T, preferred_element_type=jnp.float32)
    dw_gate = jnp.dot(x.T, d_gate, preferred_element_type=jnp.float32)
    dw_up = jnp.dot(x.T, d_up, preferred_element_type=jnp.float32)
    dw_down = jnp.dot(hidden.astype(jnp.bfloat16).T, dy, preferred_element_type=jnp.float32)
    return tuple(g.astype(jnp.bfloat16) for g in (dx, dw_gate, dw_up, dw_down))
```

```python
import functools

import jax
import jax.numpy as jnp
from jax import lax
from jax.experimental import pallas as pl
from jax.experimental.pallas import tpu as pltpu
from jax.sharding import PartitionSpec as P

BF, F32 = jnp.bfloat16, jnp.float32
NC = 4
MIB = 2**20


def nt(a, b):
    return lax.dot_general(a, b, (((1,), (1,)), ((), ())), preferred_element_type=F32)


def tn(a, b):
    return lax.dot_general(a, b, (((0,), (0,)), ((), ())), preferred_element_type=F32)


def gates(d_hidden, g, u):
    c, d = 0.7978845608028654, 0.044715
    g2 = g * g
    h = 0.5 * jnp.tanh(g * (c + (c * d) * g2)) + 0.5
    gelu = g * h
    slope = h + gelu * (1.0 - h) * (2.0 * c + (6.0 * c * d) * g2)
    return d_hidden * u * slope, d_hidden * gelu, gelu * u


def step_kernel(
    n, x, dy, gate, up, wg, wu, wd,
    dx, owg, owu, owd, kept,
    dyv, xv, gu, hb, hid,
    dy_sem, x_sem, gu_sem, kept_sem, hid_sem, w_sem, chunk_sem, send_sem, recv_sem,
):
    T, D = x.shape
    F = gate.shape[1]
    R = T // n
    H, FC, DC = R // 2, F // NC, D // NC
    me = lax.axis_index("tp")
    right, left = lax.rem(me + 1, n), lax.rem(me + n - 1, n)
    last = n - 1

    barrier = pltpu.get_barrier_semaphore()
    for peer in (left, right):
        pl.semaphore_signal(barrier, inc=1, device_id={"tp": peer})

    def rows_of(m):
        up_row = lax.rem(me + 3 * n - 1 - m, n) * R
        low_row = lax.rem(me + 1 + m, n) * R + H
        return pl.multiple_of(up_row, H), pl.multiple_of(low_row, H)

    def chunk(c, size):
        return pl.ds(pl.multiple_of(c * size, size), size)

    def load_rows(src, dst, k, sem):
        for half, row in enumerate(rows_of(k)):
            pltpu.make_async_copy(src.at[pl.ds(row, H), :], dst.at[pl.ds(pl.multiple_of(k * R + half * H, H), H), :], sem).start()

    def load_gu(k):
        slot = lax.rem(k, 2)
        for half, row in enumerate(rows_of(k)):
            for w, src in enumerate((gate, up)):
                for c in range(NC):
                    pltpu.make_async_copy(
                        src.at[pl.ds(row, H), pl.ds(c * FC, FC)],
                        gu.at[slot, pl.ds((w * NC + c) * R + half * H, H), :],
                        gu_sem.at[slot],
                    ).start()

    def wait(ref, sem):
        pltpu.make_async_copy(ref, ref, sem).wait()

    def load_w(src, dst, c, sem):
        return pltpu.make_async_copy(src.at[chunk(c, dst.shape[0] // NC), :], dst.at[chunk(c, dst.shape[0] // NC), :], sem)

    def message(m, c):
        copies = []
        for way, (row, peer) in enumerate(zip(rows_of(m), (right, left))):
            part = dx.at[pl.ds(row, H), chunk(c, DC)]
            copies.append(
                pltpu.make_async_remote_copy(
                    src_ref=part,
                    dst_ref=part,
                    send_sem=send_sem.at[way, c],
                    recv_sem=recv_sem.at[way, m, c],
                    device_id={"tp": peer},
                )
            )
        return copies

    def hidden(k, c):
        slot = lax.rem(k, 2)
        g_rows, u_rows = (pl.ds(pl.multiple_of((w * NC + c) * R, R), R) for w in range(2))
        d_hidden = nt(dyv[chunk(k, R), :], owd[chunk(c, FC), :])
        g, u = gu[slot, g_rows, :].astype(F32), gu[slot, u_rows, :].astype(F32)
        for buf, v in zip((hb.at[slot, 0], hb.at[slot, 1], hid), gates(d_hidden, g, u)):
            buf[:, chunk(c, FC)] = v.astype(BF)

    def keep(k, c):
        slot = lax.rem(k, 2)
        for w, buf in enumerate((hb.at[slot, 0], hb.at[slot, 1], hid)):
            pltpu.make_async_copy(
                buf.at[:, chunk(c, FC)],
                kept.at[w, c, chunk(k, R), :],
                hid_sem.at[c] if w == 2 else kept_sem.at[slot],
            ).start()

    def kept_hidden(c):
        wait(hid.at[:, chunk(c, FC)], hid_sem.at[c])

    def load_kept(q):
        w = lax.rem(q // NC + 2, 3)
        return pltpu.make_async_copy(kept.at[w, lax.rem(q, NC)], gu.at[lax.rem(q, 2)], chunk_sem.at[lax.rem(q, 2)])

    def load_step(k):
        load_rows(dy, dyv, k, dy_sem.at[k])
        load_gu(k)

    def loaded_step(k):
        wait(dyv.at[chunk(k, R), :], dy_sem.at[k])
        wait(gu.at[lax.rem(k, 2)], gu_sem.at[lax.rem(k, 2)])

    def term(k, c):
        slot = lax.rem(k, 2)
        return nt(hb[slot, 0], owg[chunk(c, DC), :]) + nt(hb[slot, 1], owu[chunk(c, DC), :])

    def arrived(m, c):
        for copy in message(m, c):
            copy.wait_recv()
            copy.wait_send()

    def send(m, c):
        for copy in message(m, c):
            copy.start()

    def add(k, c):
        acc = term(k, c)
        for half, row in enumerate(rows_of(k)):
            here = dx[pl.ds(row, H), chunk(c, DC)].astype(F32)
            dx[pl.ds(row, H), chunk(c, DC)] = (here + acc[half * H : (half + 1) * H, :]).astype(BF)

    down, gw, uw = (
        lambda c, w=w, src=src, dst=dst: load_w(src, dst, c, w_sem.at[w, c])
        for w, (src, dst) in enumerate(((wd, owd), (wg, owg), (wu, owu)))
    )
    load_rows(dy, dyv, 0, dy_sem.at[0])
    down(0).start()
    load_gu(0)
    down(1).start()
    loaded_step(0)
    for c in range(NC):
        down(c).wait()
        if c + 2 < NC:
            down(c + 2).start()
        elif c + 2 == NC:
            gw(0).start()
            uw(0).start()
        else:
            for b in range(1, NC):
                gw(b).start()
                uw(b).start()
            load_step(1)
        hidden(0, c)
        keep(0, c)
    pl.semaphore_wait(barrier, 2)

    def opening(c, _):
        @pl.when(c == 0)
        def _():
            loaded_step(1)
            load_step(2)

        gw(c).wait()
        uw(c).wait()
        kept_hidden(c)
        acc = term(0, c)
        for half, row in enumerate(rows_of(0)):
            dx[pl.ds(row, H), chunk(c, DC)] = acc[half * H : (half + 1) * H, :].astype(BF)
        send(0, c)
        hidden(1, c)
        keep(1, c)
        return 0

    lax.fori_loop(0, NC, opening, 0)
    load_rows(x, xv, 0, x_sem)

    def unit(i, _):
        k, c = i // NC, lax.rem(i, NC)

        @pl.when(c == 0)
        def _():
            loaded_step(k + 1)
            wait(hb.at[lax.rem(k + 1, 2)], kept_sem.at[lax.rem(k + 1, 2)])
            load_rows(x, xv, k, x_sem)

            @pl.when(k < last - 1)
            def _():
                load_step(k + 2)

        kept_hidden(c)
        arrived(k - 1, c)
        add(k, c)
        send(k, c)
        hidden(k + 1, c)
        keep(k + 1, c)
        return 0

    lax.fori_loop(NC, last * NC, unit, 0)
    load_rows(x, xv, last, x_sem)

    def closing(c, _):
        kept_hidden(c)
        arrived(last - 1, c)
        add(last, c)
        send(last, c)
        return 0

    lax.fori_loop(0, NC, closing, 0)
    for s in range(2):
        wait(hb.at[s], kept_sem.at[s])
    for s in range(2):
        load_kept(s).start()
    wait(xv, x_sem)

    def spread(i):
        m, c = n + i // NC, lax.rem(i, NC)
        arrived(m - 1, c)
        send(m, c)

    def grads(w):
        def body(j, _):
            i = w * 2 * NC + j
            q, half = i // 2, lax.rem(i, 2)
            c, slot = lax.rem(q, NC), lax.rem(q, 2)
            spread(i)

            @pl.when(half == 0)
            def _():
                load_kept(q).wait()

            side = chunk(half, D // 2)
            if w == 0:
                owd[chunk(c, FC), side] = tn(gu[slot], dyv[:, side]).astype(BF)
            else:
                (owg, owu)[w - 1][side, chunk(c, FC)] = tn(xv[:, side], gu[slot]).astype(BF)

            @pl.when(jnp.logical_and(half == 1, q < 3 * NC - 2))
            def _():
                load_kept(q + 2).start()

            return 0

        lax.fori_loop(0, 2 * NC, body, 0)

    for w in range(3):
        grads(w)
    for c in range(NC):
        arrived(2 * n - 3, c)


def store_kernel(*refs):
    count = len(refs) // 2
    sems = refs[-1]
    copies = [pltpu.make_async_copy(refs[i], refs[count + i], sems.at[i]) for i in range(count)]
    for copy in copies:
        copy.start()
    for copy in copies:
        copy.wait()


def solution(mesh):
    n = mesh.shape["tp"]

    def step(x, dy, gate, up, w_gate, w_up, w_down):
        T, D = x.shape
        F = gate.shape[1]
        R = T // n
        assert 2 * NC * R == T and (n - 2) * NC == 6 * NC
        shapes = [(T, D), (D, F), (D, F), (F, D)]
        hbm = pl.BlockSpec(memory_space=pl.ANY)
        vmem = pl.BlockSpec(memory_space=pltpu.VMEM)
        *outs, _ = pl.pallas_call(
            functools.partial(step_kernel, n),
            out_shape=[*(pltpu.VMEM(s, BF) for s in shapes), pltpu.HBM((3, NC, T, F // NC), BF)],
            in_specs=[hbm] * 7,
            out_specs=[vmem] * 4 + [hbm],
            scratch_shapes=[
                pltpu.VMEM((T, D), BF),
                pltpu.VMEM((T, D), BF),
                pltpu.VMEM((2, T, F // NC), BF),
                pltpu.VMEM((2, 2, R, F), BF),
                pltpu.VMEM((R, F), BF),
                pltpu.SemaphoreType.DMA((n,)),
                pltpu.SemaphoreType.DMA,
                pltpu.SemaphoreType.DMA((2,)),
                pltpu.SemaphoreType.DMA((2,)),
                pltpu.SemaphoreType.DMA((NC,)),
                pltpu.SemaphoreType.DMA((3, NC)),
                pltpu.SemaphoreType.DMA((2,)),
                pltpu.SemaphoreType.DMA((2, NC)),
                pltpu.SemaphoreType.DMA((2, 2 * n - 2, NC)),
            ],
            compiler_params=pltpu.CompilerParams(
                collective_id=0, has_side_effects=True, vmem_limit_bytes=30 * MIB
            ),
            name="mlp_backward",
        )(x, dy, gate, up, w_gate, w_up, w_down)
        store = lambda *o: pl.pallas_call(
            store_kernel,
            out_shape=[jax.ShapeDtypeStruct(s.shape, BF) for s in o],
            in_specs=[vmem] * len(o),
            out_specs=[hbm] * len(o),
            scratch_shapes=[pltpu.SemaphoreType.DMA((len(o),))],
            compiler_params=pltpu.CompilerParams(vmem_limit_bytes=1 * MIB),
            name="store",
        )(*o)
        dx, = store(outs[0])
        return dx, *store(*outs[1:])

    tokens, columns, rows = P("dp", None), P(None, "tp"), P("tp", None)
    return jax.shard_map(
        step,
        mesh=mesh,
        in_specs=(tokens, tokens, P("dp", "tp"), P("dp", "tp"), columns, columns, rows),
        out_specs=(tokens, P("dp", "tp"), P("dp", "tp"), P(("dp", "tp"), None)),
        check_vma=False,
    )
```

```python
import functools

import jax
import jax.numpy as jnp
from jax import lax
from jax.experimental import pallas as pl
from jax.experimental.pallas import tpu as pltpu
from jax.sharding import PartitionSpec as P

BF, F32 = jnp.bfloat16, jnp.float32
NC = 4
MIB = 2**20


def nt(a, b):
    return lax.dot_general(a, b, (((1,), (1,)), ((), ())), preferred_element_type=F32)


def tn(a, b):
    return lax.dot_general(a, b, (((0,), (0,)), ((), ())), preferred_element_type=F32)


def gates(d_hidden, g, u):
    c, d = 0.7978845608028654, 0.044715
    g2 = g * g
    h = 0.5 * jnp.tanh(g * (c + (c * d) * g2)) + 0.5
    gelu = g * h
    slope = h + gelu * (1.0 - h) * (2.0 * c + (6.0 * c * d) * g2)
    return d_hidden * u * slope, d_hidden * gelu, gelu * u


def step_kernel(
    n, x, dy, gate, up, wg, wu, wd,
    dx, owg, owu, owd, end_up, end_low, kept,
    dyv, xv, gu, hb, hid,
    dy_sem, x_sem, gu_sem, kept_sem, hid_sem, w_sem, chunk_sem, send_sem, recv_sem,
):
    T, D = x.shape
    F = gate.shape[1]
    R = T // n
    H, FC, DC = R // 2, F // NC, D // NC
    me = lax.axis_index("tp")
    right, left = lax.rem(me + 1, n), lax.rem(me + n - 1, n)
    last = n - 1

    barrier = pltpu.get_barrier_semaphore()
    for peer in (left, right):
        pl.semaphore_signal(barrier, inc=1, device_id={"tp": peer})

    def rows_of(m):
        up_row = lax.rem(me + 3 * n - 1 - m, n) * R
        low_row = lax.rem(me + 1 + m, n) * R + H
        return pl.multiple_of(up_row, H), pl.multiple_of(low_row, H)

    def chunk(c, size):
        return pl.ds(pl.multiple_of(c * size, size), size)

    def load_rows(src, dst, k, sem):
        for half, row in enumerate(rows_of(k)):
            pltpu.make_async_copy(src.at[pl.ds(row, H), :], dst.at[pl.ds(pl.multiple_of(k * R + half * H, H), H), :], sem).start()

    def load_gu(k):
        slot = lax.rem(k, 2)
        for half, row in enumerate(rows_of(k)):
            for w, src in enumerate((gate, up)):
                for c in range(NC):
                    pltpu.make_async_copy(
                        src.at[pl.ds(row, H), pl.ds(c * FC, FC)],
                        gu.at[slot, pl.ds((w * NC + c) * R + half * H, H), :],
                        gu_sem.at[slot],
                    ).start()

    def wait(ref, sem):
        pltpu.make_async_copy(ref, ref, sem).wait()

    def load_w(src, dst, c, sem):
        return pltpu.make_async_copy(src.at[chunk(c, dst.shape[0] // NC), :], dst.at[chunk(c, dst.shape[0] // NC), :], sem)

    def message(m, c):
        copies = []
        for way, (row, peer) in enumerate(zip(rows_of(m), (right, left))):
            part = dx.at[pl.ds(row, H), chunk(c, DC)]
            copies.append(
                pltpu.make_async_remote_copy(
                    src_ref=part,
                    dst_ref=part,
                    send_sem=send_sem.at[way, c],
                    recv_sem=recv_sem.at[way, m, c],
                    device_id={"tp": peer},
                )
            )
        return copies

    def hidden(k, c):
        slot = lax.rem(k, 2)
        g_rows, u_rows = (pl.ds(pl.multiple_of((w * NC + c) * R, R), R) for w in range(2))
        d_hidden = nt(dyv[chunk(k, R), :], owd[chunk(c, FC), :])
        g, u = gu[slot, g_rows, :].astype(F32), gu[slot, u_rows, :].astype(F32)
        for buf, v in zip((hb.at[slot, 0], hb.at[slot, 1], hid), gates(d_hidden, g, u)):
            buf[:, chunk(c, FC)] = v.astype(BF)

    def keep(k, c):
        slot = lax.rem(k, 2)
        for w, buf in enumerate((hb.at[slot, 0], hb.at[slot, 1], hid)):
            pltpu.make_async_copy(
                buf.at[:, chunk(c, FC)],
                kept.at[w, c, chunk(k, R), :],
                hid_sem.at[c] if w == 2 else kept_sem.at[slot],
            ).start()

    def kept_hidden(c):
        wait(hid.at[:, chunk(c, FC)], hid_sem.at[c])

    def load_kept(q):
        w = lax.rem(q // NC + 2, 3)
        return pltpu.make_async_copy(kept.at[w, lax.rem(q, NC)], gu.at[lax.rem(q, 2)], chunk_sem.at[lax.rem(q, 2)])

    def load_step(k):
        load_rows(dy, dyv, k, dy_sem.at[k])
        load_gu(k)

    def loaded_step(k):
        wait(dyv.at[chunk(k, R), :], dy_sem.at[k])
        wait(gu.at[lax.rem(k, 2)], gu_sem.at[lax.rem(k, 2)])

    def term(k, c):
        slot = lax.rem(k, 2)
        return nt(hb[slot, 0], owg[chunk(c, DC), :]) + nt(hb[slot, 1], owu[chunk(c, DC), :])

    def arrived(m, c):
        for copy in message(m, c):
            copy.wait_recv()
            copy.wait_send()

    def send(m, c):
        for copy in message(m, c):
            copy.start()

    def add(k, c):
        acc = term(k, c)
        for half, row in enumerate(rows_of(k)):
            here = dx[pl.ds(row, H), chunk(c, DC)].astype(F32)
            dx[pl.ds(row, H), chunk(c, DC)] = (here + acc[half * H : (half + 1) * H, :]).astype(BF)

    down, gw, uw = (
        lambda c, w=w, src=src, dst=dst: load_w(src, dst, c, w_sem.at[w, c])
        for w, (src, dst) in enumerate(((wd, owd), (wg, owg), (wu, owu)))
    )
    load_rows(dy, dyv, 0, dy_sem.at[0])
    down(0).start()
    load_gu(0)
    down(1).start()
    loaded_step(0)
    for c in range(NC):
        down(c).wait()
        if c + 2 < NC:
            down(c + 2).start()
        elif c + 2 == NC:
            gw(0).start()
            uw(0).start()
        else:
            for b in range(1, NC):
                gw(b).start()
                uw(b).start()
            load_step(1)
        hidden(0, c)
        keep(0, c)
    pl.semaphore_wait(barrier, 2)

    def opening(c, _):
        @pl.when(c == 0)
        def _():
            loaded_step(1)
            load_step(2)

        gw(c).wait()
        uw(c).wait()
        kept_hidden(c)
        acc = term(0, c)
        for half, row in enumerate(rows_of(0)):
            dx[pl.ds(row, H), chunk(c, DC)] = acc[half * H : (half + 1) * H, :].astype(BF)
        send(0, c)
        hidden(1, c)
        keep(1, c)
        return 0

    lax.fori_loop(0, NC, opening, 0)
    load_rows(x, xv, 0, x_sem)

    def unit(i, _):
        k, c = i // NC, lax.rem(i, NC)

        @pl.when(c == 0)
        def _():
            loaded_step(k + 1)
            wait(hb.at[lax.rem(k + 1, 2)], kept_sem.at[lax.rem(k + 1, 2)])
            load_rows(x, xv, k, x_sem)

            @pl.when(k < last - 1)
            def _():
                load_step(k + 2)

        kept_hidden(c)
        arrived(k - 1, c)
        add(k, c)
        send(k, c)
        hidden(k + 1, c)
        keep(k + 1, c)
        return 0

    lax.fori_loop(NC, last * NC, unit, 0)
    load_rows(x, xv, last, x_sem)

    def closing(c, _):
        kept_hidden(c)
        arrived(last - 1, c)
        add(last, c)
        send(last, c)
        return 0

    lax.fori_loop(0, NC, closing, 0)
    for s in range(2):
        wait(hb.at[s], kept_sem.at[s])
    for s in range(2):
        load_kept(s).start()
    wait(xv, x_sem)

    def spread(i):
        m, c = n + i // NC, lax.rem(i, NC)
        arrived(m - 1, c)
        send(m, c)

    def grads(w):
        def body(j, _):
            i = w * 2 * NC + j
            q, half = i // 2, lax.rem(i, 2)
            c, slot = lax.rem(q, NC), lax.rem(q, 2)
            @pl.when(i < (n - 3) * NC)
            def _():
                spread(i)

            @pl.when(half == 0)
            def _():
                load_kept(q).wait()

            side = chunk(half, D // 2)
            if w == 0:
                owd[chunk(c, FC), side] = tn(gu[slot], dyv[:, side]).astype(BF)
            else:
                (owg, owu)[w - 1][side, chunk(c, FC)] = tn(xv[:, side], gu[slot]).astype(BF)

            @pl.when(jnp.logical_and(half == 1, q < 3 * NC - 2))
            def _():
                load_kept(q + 2).start()

            return 0

        lax.fori_loop(0, 2 * NC, body, 0)

    for w in range(3):
        grads(w)
    for c in range(NC):
        arrived(2 * n - 4, c)
        for end, row in zip((end_up, end_low), rows_of(2 * n - 3)):
            end[:, pl.ds(c * DC, DC)] = dx[pl.ds(row, H), pl.ds(c * DC, DC)]


def store_kernel(*refs):
    count = len(refs) // 2
    sems = refs[-1]
    copies = [pltpu.make_async_copy(refs[i], refs[count + i], sems.at[i]) for i in range(count)]
    for copy in copies:
        copy.start()
    for copy in copies:
        copy.wait()


def merge_kernel(n, got_up, got_low, _, dx, sems):
    H, me = got_up.shape[0], lax.axis_index("tp")
    rows = lax.rem(me + 1, n) * 2 * H, lax.rem(me + n - 1, n) * 2 * H + H
    copies = [
        pltpu.make_async_copy(got, dx.at[pl.ds(pl.multiple_of(row, H), H), :], sems.at[i])
        for i, (got, row) in enumerate(zip((got_up, got_low), rows))
    ]
    for copy in copies:
        copy.start()
    for copy in copies:
        copy.wait()


def solution(mesh):
    n = mesh.shape["tp"]

    def step(x, dy, gate, up, w_gate, w_up, w_down):
        T, D = x.shape
        F = gate.shape[1]
        R = T // n
        assert 2 * NC * R == T and (n - 2) * NC == 6 * NC
        shapes = [(T, D), (D, F), (D, F), (F, D)]
        end = (R // 2, D)
        hbm = pl.BlockSpec(memory_space=pl.ANY)
        vmem = pl.BlockSpec(memory_space=pltpu.VMEM)
        *outs, end_up, end_low, _ = pl.pallas_call(
            functools.partial(step_kernel, n),
            out_shape=[*(pltpu.VMEM(s, BF) for s in (*shapes, end, end)), pltpu.HBM((3, NC, T, F // NC), BF)],
            in_specs=[hbm] * 7,
            out_specs=[vmem] * 6 + [hbm],
            scratch_shapes=[
                pltpu.VMEM((T, D), BF),
                pltpu.VMEM((T, D), BF),
                pltpu.VMEM((2, T, F // NC), BF),
                pltpu.VMEM((2, 2, R, F), BF),
                pltpu.VMEM((R, F), BF),
                pltpu.SemaphoreType.DMA((n,)),
                pltpu.SemaphoreType.DMA,
                pltpu.SemaphoreType.DMA((2,)),
                pltpu.SemaphoreType.DMA((2,)),
                pltpu.SemaphoreType.DMA((NC,)),
                pltpu.SemaphoreType.DMA((3, NC)),
                pltpu.SemaphoreType.DMA((2,)),
                pltpu.SemaphoreType.DMA((2, NC)),
                pltpu.SemaphoreType.DMA((2, 2 * n - 3, NC)),
            ],
            compiler_params=pltpu.CompilerParams(
                collective_id=0, has_side_effects=True, vmem_limit_bytes=30 * MIB
            ),
            name="mlp_backward",
        )(x, dy, gate, up, w_gate, w_up, w_down)
        store = lambda *o: pl.pallas_call(
            store_kernel,
            out_shape=[jax.ShapeDtypeStruct(s.shape, BF) for s in o],
            in_specs=[vmem] * len(o),
            out_specs=[hbm] * len(o),
            scratch_shapes=[pltpu.SemaphoreType.DMA((len(o),))],
            compiler_params=pltpu.CompilerParams(vmem_limit_bytes=1 * MIB),
            cost_estimate=pl.CostEstimate(flops=2**31 * len(o), bytes_accessed=4 * T * D * len(o), transcendentals=0),
            name="store",
        )(*o)
        got_up = lax.ppermute(end_up, "tp", [(i, (i + 1) % n) for i in range(n)])
        got_low = lax.ppermute(end_low, "tp", [(i, (i - 1) % n) for i in range(n)])
        (dx,) = store(outs[0])
        grads = store(*outs[1:])
        dx = pl.pallas_call(
            functools.partial(merge_kernel, n),
            out_shape=jax.ShapeDtypeStruct(dx.shape, BF),
            in_specs=[vmem, vmem, hbm],
            out_specs=hbm,
            scratch_shapes=[pltpu.SemaphoreType.DMA((2,))],
            input_output_aliases={2: 0},
            compiler_params=pltpu.CompilerParams(vmem_limit_bytes=2 * MIB),
            name="merge",
        )(got_up, got_low, dx)
        return dx, *grads

    tokens, columns, rows = P("dp", None), P(None, "tp"), P("tp", None)
    return jax.shard_map(
        step,
        mesh=mesh,
        in_specs=(tokens, tokens, P("dp", "tp"), P("dp", "tp"), columns, columns, rows),
        out_specs=(tokens, P("dp", "tp"), P("dp", "tp"), P(("dp", "tp"), None)),
        check_vma=False,
    )
```

```python
import functools

import jax
import jax.numpy as jnp
from jax import lax
from jax.experimental import pallas as pl
from jax.experimental.pallas import tpu as pltpu
from jax.sharding import PartitionSpec as P

BF, F32 = jnp.bfloat16, jnp.float32
NC = 4
MIB = 2**20


def nt(a, b):
    return lax.dot_general(a, b, (((1,), (1,)), ((), ())), preferred_element_type=F32)


def tn(a, b):
    return lax.dot_general(a, b, (((0,), (0,)), ((), ())), preferred_element_type=F32)


def gates(d_hidden, g, u):
    c, d = 0.7978845608028654, 0.044715
    g2 = g * g
    h = 0.5 * jnp.tanh(g * (c + (c * d) * g2)) + 0.5
    gelu = g * h
    slope = h + gelu * (1.0 - h) * (2.0 * c + (6.0 * c * d) * g2)
    return d_hidden * u * slope, d_hidden * gelu, gelu * u


def step_kernel(
    n, x, dy, gate, up, wg, wu, wd,
    dx, owg, owu, owd, end_up, end_low, kept,
    dyv, xv, gu, hb, hid,
    dy_sem, x_sem, gu_sem, kept_sem, hid_sem, w_sem, chunk_sem, send_sem, recv_sem,
):
    T, D = x.shape
    F = gate.shape[1]
    R = T // n
    H, FC, DC = R // 2, F // NC, D // NC
    me = lax.axis_index("tp")
    right, left = lax.rem(me + 1, n), lax.rem(me + n - 1, n)
    last = n - 1

    barrier = pltpu.get_barrier_semaphore()
    for peer in (left, right):
        pl.semaphore_signal(barrier, inc=1, device_id={"tp": peer})

    def rows_of(m):
        up_row = lax.rem(me + 3 * n - 1 - m, n) * R
        low_row = lax.rem(me + 1 + m, n) * R + H
        return pl.multiple_of(up_row, H), pl.multiple_of(low_row, H)

    def chunk(c, size):
        return pl.ds(pl.multiple_of(c * size, size), size)

    def load_rows(src, dst, k, sem):
        for half, row in enumerate(rows_of(k)):
            pltpu.make_async_copy(src.at[pl.ds(row, H), :], dst.at[pl.ds(pl.multiple_of(k * R + half * H, H), H), :], sem).start()

    def load_gu(k):
        slot = lax.rem(k, 2)
        for half, row in enumerate(rows_of(k)):
            for w, src in enumerate((gate, up)):
                for c in range(NC):
                    pltpu.make_async_copy(
                        src.at[pl.ds(row, H), pl.ds(c * FC, FC)],
                        gu.at[slot, pl.ds((w * NC + c) * R + half * H, H), :],
                        gu_sem.at[slot],
                    ).start()

    def wait(ref, sem):
        pltpu.make_async_copy(ref, ref, sem).wait()

    def load_w(src, dst, c, sem):
        return pltpu.make_async_copy(src.at[chunk(c, dst.shape[0] // NC), :], dst.at[chunk(c, dst.shape[0] // NC), :], sem)

    def message(m, c, columns=None):
        copies = []
        for way, (row, peer) in enumerate(zip(rows_of(m), (right, left))):
            part = dx.at[pl.ds(row, H), chunk(c, DC) if columns is None else columns]
            copies.append(
                pltpu.make_async_remote_copy(
                    src_ref=part,
                    dst_ref=part,
                    send_sem=send_sem.at[way, c],
                    recv_sem=recv_sem.at[way, m, c],
                    device_id={"tp": peer},
                )
            )
        return copies

    def hidden(k, c):
        slot = lax.rem(k, 2)
        g_rows, u_rows = (pl.ds(pl.multiple_of((w * NC + c) * R, R), R) for w in range(2))
        d_hidden = nt(dyv[chunk(k, R), :], owd[chunk(c, FC), :])
        g, u = gu[slot, g_rows, :].astype(F32), gu[slot, u_rows, :].astype(F32)
        for buf, v in zip((hb.at[slot, 0], hb.at[slot, 1], hid), gates(d_hidden, g, u)):
            buf[:, chunk(c, FC)] = v.astype(BF)

    def keep(k, c):
        slot = lax.rem(k, 2)
        for w, buf in enumerate((hb.at[slot, 0], hb.at[slot, 1], hid)):
            pltpu.make_async_copy(
                buf.at[:, chunk(c, FC)],
                kept.at[w, c, chunk(k, R), :],
                hid_sem.at[c] if w == 2 else kept_sem.at[slot],
            ).start()

    def kept_hidden(c):
        wait(hid.at[:, chunk(c, FC)], hid_sem.at[c])

    def load_kept(q):
        w = lax.rem(q // NC + 2, 3)
        return pltpu.make_async_copy(kept.at[w, lax.rem(q, NC)], gu.at[lax.rem(q, 2)], chunk_sem.at[lax.rem(q, 2)])

    def load_step(k):
        load_rows(dy, dyv, k, dy_sem.at[k])
        load_gu(k)

    def loaded_step(k):
        wait(dyv.at[chunk(k, R), :], dy_sem.at[k])
        wait(gu.at[lax.rem(k, 2)], gu_sem.at[lax.rem(k, 2)])

    def term(k, c):
        slot = lax.rem(k, 2)
        return nt(hb[slot, 0], owg[chunk(c, DC), :]) + nt(hb[slot, 1], owu[chunk(c, DC), :])

    def arrived(m, c):
        for copy in message(m, c):
            copy.wait_recv()
            copy.wait_send()

    def send(m, c):
        for copy in message(m, c):
            copy.start()

    def add(k, c):
        acc = term(k, c)
        for half, row in enumerate(rows_of(k)):
            here = dx[pl.ds(row, H), chunk(c, DC)].astype(F32)
            dx[pl.ds(row, H), chunk(c, DC)] = (here + acc[half * H : (half + 1) * H, :]).astype(BF)

    down, gw, uw = (
        lambda c, w=w, src=src, dst=dst: load_w(src, dst, c, w_sem.at[w, c])
        for w, (src, dst) in enumerate(((wd, owd), (wg, owg), (wu, owu)))
    )
    load_rows(dy, dyv, 0, dy_sem.at[0])
    down(0).start()
    load_gu(0)
    loaded_step(0)
    down(0).wait()
    later = [(down(1), down(2)), (down(3), gw(0), uw(0)), (), [b(c) for c in range(1, NC) for b in (gw, uw)]]
    for c in range(NC):
        for load in later[c]:
            load.start()
        if c == 2:
            load_step(1)
        hidden(0, c)
        keep(0, c)
        if c + 1 < NC:
            down(c + 1).wait()
    pl.semaphore_wait(barrier, 2)

    def opening(c, _):
        gw(c).wait()
        uw(c).wait()
        acc = term(0, c)
        for half, row in enumerate(rows_of(0)):
            dx[pl.ds(row, H), chunk(c, DC)] = acc[half * H : (half + 1) * H, :].astype(BF)
        send(0, c)

        @pl.when(c == 0)
        def _():
            loaded_step(1)
            load_step(2)

        kept_hidden(c)
        hidden(1, c)
        keep(1, c)
        return 0

    lax.fori_loop(0, NC, opening, 0)
    load_rows(x, xv, 0, x_sem)

    def unit(i, _):
        k, c = i // NC, lax.rem(i, NC)

        @pl.when(c == 0)
        def _():
            loaded_step(k + 1)
            wait(hb.at[lax.rem(k + 1, 2)], kept_sem.at[lax.rem(k + 1, 2)])
            load_rows(x, xv, k, x_sem)

            @pl.when(k < last - 1)
            def _():
                load_step(k + 2)

        kept_hidden(c)
        arrived(k - 1, c)
        add(k, c)
        send(k, c)
        hidden(k + 1, c)
        keep(k + 1, c)
        return 0

    lax.fori_loop(NC, last * NC, unit, 0)
    load_rows(x, xv, last, x_sem)

    def grad(w, j):
        c, half = j // 2, lax.rem(j, 2)
        q = w * NC + c
        slot = lax.rem(q, 2)

        @pl.when(half == 0)
        def _():
            load_kept(q).wait()

        side = chunk(half, D // 2)
        if w == 0:
            owd[chunk(c, FC), side] = tn(gu[slot], dyv[:, side]).astype(BF)
        else:
            (owg, owu)[w - 1][side, chunk(c, FC)] = tn(xv[:, side], gu[slot]).astype(BF)

        @pl.when(jnp.logical_and(half == 1, q < 3 * NC - 2))
        def _():
            load_kept(q + 2).start()

    def closing(c, _):
        arrived(last - 1, c)
        add(last, c)
        send(last, c)

        @pl.when(c == 0)
        def _():
            for b in range(NC):
                kept_hidden(b)
            for s in range(2):
                wait(hb.at[s], kept_sem.at[s])
            for s in range(2):
                load_kept(s).start()

        @pl.when(lax.rem(c, 2) == 1)
        def _():
            grad(0, c // 2)

        return 0

    lax.fori_loop(0, NC, closing, 0)

    early = NC // 2

    def grads(w):
        def body(j, _):
            i = w * 2 * NC + j - early

            @pl.when(i < (n - 3) * NC)
            def _():
                m, c = n + i // NC, lax.rem(i, NC)
                arrived(m - 1, c)
                send(m, c)

            grad(w, j)
            return 0

        lax.fori_loop(0 if w else early, 2 * NC, body, 0)

    grads(0)
    wait(xv, x_sem)
    grads(1)
    grads(2)
    for c in range(NC):
        arrived(2 * n - 4, c)
        for end, row in zip((end_up, end_low), rows_of(2 * n - 3)):
            end[:, pl.ds(c * DC, DC)] = dx[pl.ds(row, H), pl.ds(c * DC, DC)]


def store_kernel(*refs):
    count = len(refs) // 2
    sems = refs[-1]
    copies = [pltpu.make_async_copy(refs[i], refs[count + i], sems.at[i]) for i in range(count)]
    for copy in copies:
        copy.start()
    for copy in copies:
        copy.wait()


def merge_kernel(n, got_up, got_low, _, dx, sems):
    H, me = got_up.shape[0], lax.axis_index("tp")
    rows = lax.rem(me + 1, n) * 2 * H, lax.rem(me + n - 1, n) * 2 * H + H
    copies = [
        pltpu.make_async_copy(got, dx.at[pl.ds(pl.multiple_of(row, H), H), :], sems.at[i])
        for i, (got, row) in enumerate(zip((got_up, got_low), rows))
    ]
    for copy in copies:
        copy.start()
    for copy in copies:
        copy.wait()


def solution(mesh):
    n = mesh.shape["tp"]

    def step(x, dy, gate, up, w_gate, w_up, w_down):
        T, D = x.shape
        F = gate.shape[1]
        R = T // n
        assert 2 * NC * R == T and (n - 2) * NC == 6 * NC
        shapes = [(T, D), (D, F), (D, F), (F, D)]
        end = (R // 2, D)
        hbm = pl.BlockSpec(memory_space=pl.ANY)
        vmem = pl.BlockSpec(memory_space=pltpu.VMEM)
        *outs, end_up, end_low, _ = pl.pallas_call(
            functools.partial(step_kernel, n),
            out_shape=[*(pltpu.VMEM(s, BF) for s in (*shapes, end, end)), pltpu.HBM((3, NC, T, F // NC), BF)],
            in_specs=[hbm] * 7,
            out_specs=[vmem] * 6 + [hbm],
            scratch_shapes=[
                pltpu.VMEM((T, D), BF),
                pltpu.VMEM((T, D), BF),
                pltpu.VMEM((2, T, F // NC), BF),
                pltpu.VMEM((2, 2, R, F), BF),
                pltpu.VMEM((R, F), BF),
                pltpu.SemaphoreType.DMA((n,)),
                pltpu.SemaphoreType.DMA,
                pltpu.SemaphoreType.DMA((2,)),
                pltpu.SemaphoreType.DMA((2,)),
                pltpu.SemaphoreType.DMA((NC,)),
                pltpu.SemaphoreType.DMA((3, NC)),
                pltpu.SemaphoreType.DMA((2,)),
                pltpu.SemaphoreType.DMA((2, NC)),
                pltpu.SemaphoreType.DMA((2, 2 * n - 3, NC)),
            ],
            compiler_params=pltpu.CompilerParams(
                collective_id=0, has_side_effects=True, vmem_limit_bytes=30 * MIB,
            ),
            name="mlp_backward",
        )(x, dy, gate, up, w_gate, w_up, w_down)
        store = lambda *o: pl.pallas_call(
            store_kernel,
            out_shape=[jax.ShapeDtypeStruct(s.shape, BF) for s in o],
            in_specs=[vmem] * len(o),
            out_specs=[hbm] * len(o),
            scratch_shapes=[pltpu.SemaphoreType.DMA((len(o),))],
            compiler_params=pltpu.CompilerParams(vmem_limit_bytes=1 * MIB),
            cost_estimate=pl.CostEstimate(flops=2**31 * len(o), bytes_accessed=4 * T * D * len(o), transcendentals=0),
            name="store",
        )(*o)
        got_up = lax.ppermute(end_up, "tp", [(i, (i + 1) % n) for i in range(n)])
        got_low = lax.ppermute(end_low, "tp", [(i, (i - 1) % n) for i in range(n)])
        (dx,) = store(outs[0])
        grads = store(*outs[1:])
        dx = pl.pallas_call(
            functools.partial(merge_kernel, n),
            out_shape=jax.ShapeDtypeStruct(dx.shape, BF),
            in_specs=[vmem, vmem, hbm],
            out_specs=hbm,
            scratch_shapes=[pltpu.SemaphoreType.DMA((2,))],
            input_output_aliases={2: 0},
            compiler_params=pltpu.CompilerParams(vmem_limit_bytes=2 * MIB),
            name="merge",
        )(got_up, got_low, dx)
        return dx, *grads

    tokens, columns, rows = P("dp", None), P(None, "tp"), P("tp", None)
    return jax.shard_map(
        step,
        mesh=mesh,
        in_specs=(tokens, tokens, P("dp", "tp"), P("dp", "tp"), columns, columns, rows),
        out_specs=(tokens, P("dp", "tp"), P("dp", "tp"), P(("dp", "tp"), None)),
        check_vma=False,
    )
```
